32 devices in a mesh: lon: 16 (over z, y, core), band: 2 (over x).
Axes of the slice: x: 2, y: 2, z: 4, core: 2. Of those that a mesh axis runs over, the one named last changes fastest.
Arguments:
- nest_field: float32 [32, 96, 9216], P(None, 'band', 'lon'), may hold values from -6 to 6
- nest_area: float32 [96, 9216], P('band', 'lon'), may hold values from 0.5 to 2
- parent_field: float32 [32, 32, 3072], P(None, 'band', 'lon'), may hold values from -6 to 6
- nest_offset: int32 [1], replicated, may hold values from 576 to 9215
- relax_rate: float32 [32], replicated, may hold values from 0.3 to 0.8
- zonal_coef: float32 [32], replicated, may hold values from 0.05 to 0.24
- merid_coef: float32 [32], replicated, may hold values from 0.05 to 0.24
Outputs:
- parent_out: float32 [32, 32, 3072], P(None, 'band', 'lon')
The draws below stay inside these ranges and needn't reach their ends.
All inputs are finite; a program needn't handle non-finite values.
Results may differ from the reference program's by a relative error of at most 0.000084.
Values sent between devices are 32-bit elements; how exact they have to be, the bound alone decides.
A program may use at most 64 MiB of HBM per device.

```python
import math
import jax
import jax.numpy as jnp

NXP = 3072
LV = 32
NS = 3
NYP = 32
NYN = 96
NXN = 9216
N_LON = 16


def block_levels(stream_key, shape, split, low, largest):
    def one(axis_at, blocks):
        draws = jax.random.uniform(jax.random.fold_in(jax.random.fold_in(stream_key, 6), axis_at), (blocks,), jnp.float32, low / len(split), largest / len(split))
        return jnp.repeat(jnp.exp(draws), shape[axis_at] // blocks).reshape((-1,) + (1,) * (len(shape) - axis_at - 1))

    level = one(*split[0])
    for cut in split[1:]:
        level = level * one(*cut)
    return level


def centred(key, shape, scale, bound, cuts=(), kind=jnp.bfloat16):
    factor_of = block_levels(key, shape, cuts, -0.22, 0.18) if cuts else 1.0
    result = jax.random.normal(key, shape, jnp.float32) * scale * factor_of
    return jnp.minimum(jnp.maximum(result, -bound), bound).astype(kind)


def setup_inputs(seed: int = 0) -> dict:
    streams_of = jax.random.split(jax.random.key(seed), 8)
    return {
        "nest_field": centred(streams_of[0], (LV, NYN, NXN), 1.0, 6.0, ((1, 2), (2, 16)), jnp.float32),
        "nest_area": jnp.clip(jnp.exp(math.log(2.0) - 1.3862944 * jax.random.uniform(streams_of[1], (NYN, NXN), jnp.float32) ** block_levels(streams_of[1], (NYN, NXN), ((0, 2), (1, 16)), -0.2, 0.2)), 0.5, 2.0),
        "parent_field": centred(streams_of[2], (LV, NYP, NXP), 1.0, 6.0, ((1, 2), (2, 16)), jnp.float32),
        "nest_offset": jax.random.randint(streams_of[3], (1,), 3 * NXP // N_LON, 3 * NXP).astype(jnp.int32),
        "relax_rate": jnp.clip(jax.random.uniform(streams_of[4], (LV,), jnp.float32, 0.3, 0.8), 0.3, 0.8),
        "zonal_coef": jnp.clip(jax.random.uniform(streams_of[5], (LV,), jnp.float32, 0.05, 0.24), 0.05, 0.24),
        "merid_coef": jnp.clip(jax.random.uniform(streams_of[6], (LV,), jnp.float32, 0.05, 0.24), 0.05, 0.24),
    }


def zonal_pass(field, coef):
    left = jnp.roll(field, 1, axis=2)
    right = jnp.roll(field, -1, axis=2)
    return field + coef[:, None, None] * (left - 2.0 * field + right)


def merid_pass(field, coef):
    padded = jnp.pad(field, ((0, 0), (1, 1), (0, 0)))
    return field + coef[:, None, None] * (padded[:, :-2] - 2.0 * field + padded[:, 2:])


def reference(nest_field, nest_area, parent_field, nest_offset, relax_rate, zonal_coef, merid_coef):
    offset_cells = nest_offset[0]
    stacked = jnp.concatenate([nest_field * nest_area[None], nest_area[None]], axis=0)
    planes = stacked.shape[0]
    row_sums = stacked.reshape(planes, NYP, 3, NXN).sum(axis=2)
    rolled = jnp.roll(row_sums, offset_cells, axis=2)
    cell_sums = rolled.reshape(planes, NYP, NXP, 3).sum(axis=3)
    restricted = cell_sums[:LV] / cell_sums[LV][None]
    field = parent_field + relax_rate[:, None, None] * (restricted - parent_field)
    for sweep in range(NS):
        field = zonal_pass(field, zonal_coef)
        field = merid_pass(field, merid_coef)
    return field
```

```python
import functools

import jax
import jax.numpy as jnp
from jax import lax
from jax.experimental import pallas as pl
from jax.experimental.pallas import tpu as pltpu
from jax.sharding import PartitionSpec as P

NS = 3
HALO = NS
LANES = 128
MESH = pl.DeviceIdType.MESH


def chunk_width(par_cols):
    return max(w for w in range(1, 65) if par_cols % w == 0)


def front_kernel(width, off_ref, nest_ref, area_ref, out_ref, select, sums):
    block = pl.program_id(0)
    per, rows, cols = nest_ref.shape
    chunks = out_ref.shape[0]
    half = out_ref.shape[2]
    offset = off_ref[0]

    def place(values, first, count):
        values = values.reshape(count * rows, cols)
        high = values.astype(jnp.bfloat16)
        low = (values - high.astype(jnp.float32)).astype(jnp.bfloat16)
        by_column = jnp.dot(high, select[...], preferred_element_type=jnp.float32) + jnp.dot(
            low, select[...], preferred_element_type=jnp.float32
        )
        third = count * rows // 3
        tiles = []
        for t in range(sums.shape[0]):
            sums[t, : count * rows] = by_column[:, t * LANES : (t + 1) * LANES]
            tiles.append(
                sums.at[t][pl.ds(0, third, stride=3), :]
                + sums.at[t][pl.ds(1, third, stride=3), :]
                + sums.at[t][pl.ds(2, third, stride=3), :]
            )
        total = jnp.concatenate(tiles, axis=1).reshape(count, 2 * half, LANES * len(tiles))
        for c in range(chunks):
            part = total[:, :, c * width : (c + 1) * width]
            packed = jnp.concatenate([part[:, :half], part[:, half:]], axis=2)
            out_ref[c, pl.ds(first, count)] = packed

    @pl.when(block == 0)
    def _():
        slot = lax.broadcasted_iota(jnp.int32, select.shape, 1)
        cell = lax.broadcasted_iota(jnp.int32, select.shape, 0)
        lowest = (slot - offset // 3 % width) * 3 - offset % 3
        hit = (cell >= lowest) & (cell < lowest + 3)
        select[...] = jnp.where(hit, 1.0, 0.0).astype(jnp.bfloat16)
        place(area_ref[...][None], out_ref.shape[1] - 1, 1)

    place(nest_ref[...] * area_ref[...][None], block * per, per)


def front(nest_field, nest_area, nest_offset, width, chunks):
    levels, rows, cols = nest_field.shape
    half = rows // 6
    per = 8
    tiles = (chunks * width + LANES - 1) // LANES
    return pl.pallas_call(
        functools.partial(front_kernel, width),
        grid=(levels // per,),
        out_shape=jax.ShapeDtypeStruct((chunks, levels + 1, half, 2 * width), jnp.float32),
        in_specs=[
            pl.BlockSpec(memory_space=pltpu.SMEM),
            pl.BlockSpec((per, rows, cols), lambda b: (b, 0, 0)),
            pl.BlockSpec((rows, cols), lambda b: (0, 0)),
        ],
        out_specs=pl.BlockSpec((chunks, levels + 1, half, 2 * width), lambda b: (0, 0, 0, 0)),
        scratch_shapes=[
            pltpu.VMEM((cols, tiles * LANES), jnp.bfloat16),
            pltpu.VMEM((tiles, per * rows, LANES), jnp.float32),
        ],
        compiler_params=pltpu.CompilerParams(dimension_semantics=("arbitrary",)),
    )(nest_offset, nest_field, nest_area)


def send_on(value, steps):
    count = lax.axis_size("lon")
    if steps % count == 0:
        return value
    return lax.ppermute(value, "lon", [(i, (i + steps) % count) for i in range(count)])


def moved(partial, place, per_device):
    steps, slot = divmod(place, per_device)
    near = send_on(partial[: per_device - slot], steps)
    far = send_on(partial[per_device - slot :], steps + 1)
    shared = near[:1] + far[slot:]
    return jnp.concatenate([far[:slot], shared, near[1:]], axis=0)


def tail_kernel(
    sums_ref, parent_ref, relax_ref, zonal_ref, merid_ref, out_ref,
    field, west_out, east_out, first_out, last_out, west_in, east_in, above_in, below_in,
    send_sems, recv_sems,
):
    lon, band = lax.axis_index("lon"), lax.axis_index("band")
    lons, bands = lax.axis_size("lon"), lax.axis_size("band")
    levels, rows, cols = parent_ref.shape
    lanes = field.shape[2]
    chunks, _, half, double = sums_ref.shape
    width = double // 2
    west, east = lax.rem(lon + lons - 1, lons), lax.rem(lon + 1, lons)
    has_above, has_below = band > 0, band < bands - 1

    barrier = pltpu.get_barrier_semaphore()

    def greet(x, y):
        pl.semaphore_signal(barrier, inc=1, device_id=(x, y), device_id_type=MESH)

    greet(west, band)
    greet(east, band)

    @pl.when(has_above)
    def _():
        for x in (west, lon, east):
            greet(x, band - 1)

    @pl.when(has_below)
    def _():
        for x in (west, lon, east):
            greet(x, band + 1)

    lane = lax.broadcasted_iota(jnp.int32, (rows, LANES), 1)

    def blend(level, edges):
        west_edge, east_edge = edges
        top, bottom = [], []
        for c in range(chunks):
            ratio = sums_ref[c, level] / sums_ref[c, levels]
            top.append(ratio[:, :width])
            bottom.append(ratio[:, width:])
        restricted = jnp.concatenate(
            [jnp.concatenate(top, axis=1), jnp.concatenate(bottom, axis=1)], axis=0
        )
        parent = parent_ref[level]
        value = parent + relax_ref[level] * (restricted - parent)
        value = jnp.concatenate(
            [value, jnp.zeros((rows, lanes - cols), jnp.float32)], axis=1
        )
        field[level] = value
        for k in range(HALO):
            first_out[k, pl.ds(level, 1), :] = value[k : k + 1]
            last_out[k, pl.ds(level, 1), :] = value[rows - HALO + k : rows - HALO + k + 1]
        mine = lane // 4 == level
        at = (cols - HALO) // LANES * LANES
        west_edge = jnp.where(mine, pltpu.roll(value[:, :LANES], 4 * level, 1), west_edge)
        east_edge = jnp.where(
            mine,
            pltpu.roll(
                value[:, at : at + LANES],
                lax.rem(4 * level + LANES - (cols - HALO - at), LANES),
                1,
            ),
            east_edge,
        )
        return west_edge, east_edge

    empty = jnp.zeros((rows, LANES), jnp.float32)
    west_edge, east_edge = lax.fori_loop(0, levels, blend, (empty, empty))
    west_out[...] = west_edge
    east_out[...] = east_edge

    pl.semaphore_wait(
        barrier, 2 + 3 * has_above.astype(jnp.int32) + 3 * has_below.astype(jnp.int32)
    )

    def copy(index, source, target, x, y):
        return pltpu.make_async_remote_copy(
            src_ref=source,
            dst_ref=target,
            send_sem=send_sems.at[index],
            recv_sem=recv_sems.at[index],
            device_id=(x, y),
            device_id_type=MESH,
        )

    same = [
        copy(0, west_out, east_in.at[0], west, band),
        copy(1, east_out, west_in.at[0], east, band),
    ]
    upward = [
        copy(2, first_out, below_in, lon, band - 1),
        copy(3, west_out, east_in.at[2], west, band - 1),
        copy(4, east_out, west_in.at[2], east, band - 1),
    ]
    downward = [
        copy(5, last_out, above_in, lon, band + 1),
        copy(6, west_out, east_in.at[1], west, band + 1),
        copy(7, east_out, west_in.at[1], east, band + 1),
    ]

    @pl.when(has_above)
    def _():
        for one in upward:
            one.start()

    @pl.when(has_below)
    def _():
        for one in downward:
            one.start()

    for one in same:
        one.start()

    @pl.when(jnp.logical_not(has_above))
    def _():
        above_in[...] = jnp.zeros_like(above_in)
        east_in[1] = empty
        west_in[1] = empty

    @pl.when(jnp.logical_not(has_below))
    def _():
        below_in[...] = jnp.zeros_like(below_in)
        east_in[2] = empty
        west_in[2] = empty

    for one in same:
        one.wait_recv()

    @pl.when(has_above)
    def _():
        for one in downward:
            one.wait_recv()

    @pl.when(has_below)
    def _():
        for one in upward:
            one.wait_recv()

    tall = rows + 8
    sub = lax.broadcasted_iota(jnp.int32, (8, LANES), 0)

    def column_of(ref):
        corner = jnp.where(
            sub < HALO, ref[2, :8], jnp.where(sub >= 8 - HALO, ref[1, rows - 8 :], 0.0)
        )
        return jnp.concatenate([ref[0], corner], axis=0)

    east_cols, west_cols = column_of(east_in), column_of(west_in)
    row = lax.broadcasted_iota(jnp.int32, (tall, lanes), 0)
    valid = (
        (row < rows)
        | ((row < rows + HALO) & has_below)
        | ((row >= tall - HALO) & has_above)
    )
    wide = lax.broadcasted_iota(jnp.int32, (tall, LANES), 1)
    head = lanes - LANES
    spare = jnp.zeros((8 - 2 * HALO, lanes), jnp.float32)

    def smooth(level, carry):
        extra = [below_in[k, pl.ds(level, 1), :] for k in range(HALO)] + [spare]
        extra += [above_in[k, pl.ds(level, 1), :] for k in range(HALO)]
        value = jnp.concatenate([field[level]] + extra, axis=0)
        right = pltpu.roll(east_cols, lax.rem(cols - head + LANES - 4 * level, LANES), 1)
        left = pltpu.roll(west_cols, lax.rem(2 * LANES - HALO - 4 * level, LANES), 1)
        tile = value[:, head:]
        tile = jnp.where((wide >= cols - head) & (wide < cols - head + HALO), right, tile)
        tile = jnp.where(wide >= LANES - HALO, left, tile)
        if head:
            tile = jnp.concatenate([value[:, :head], tile], axis=1)
        value = tile
        zonal, merid = zonal_ref[level], merid_ref[level]
        for sweep in range(NS):
            sides = pltpu.roll(value, 1, 1) + pltpu.roll(value, lanes - 1, 1)
            value = value + zonal * (sides - 2.0 * value)
            sides = pltpu.roll(value, 1, 0) + pltpu.roll(value, tall - 1, 0)
            value = jnp.where(valid, value + merid * (sides - 2.0 * value), 0.0)
        out_ref[level] = value[:rows, :cols]
        return carry

    lax.fori_loop(0, levels, smooth, 0)

    for one in same:
        one.wait_send()

    @pl.when(has_above)
    def _():
        for one in upward:
            one.wait_send()

    @pl.when(has_below)
    def _():
        for one in downward:
            one.wait_send()


def tail(sums, parent_field, relax_rate, zonal_coef, merid_coef):
    levels, rows, cols = parent_field.shape
    lanes = (cols + 2 * HALO + LANES - 1) // LANES * LANES
    assert 4 * levels <= LANES and cols - (lanes - LANES) >= HALO
    vmem, smem = pl.BlockSpec(memory_space=pltpu.VMEM), pl.BlockSpec(memory_space=pltpu.SMEM)
    edge = pltpu.VMEM((rows, LANES), jnp.float32)
    edges = pltpu.VMEM((3, rows, LANES), jnp.float32)
    strip = pltpu.VMEM((HALO, levels, lanes), jnp.float32)
    return pl.pallas_call(
        tail_kernel,
        out_shape=jax.ShapeDtypeStruct(parent_field.shape, jnp.float32),
        in_specs=[vmem, vmem, smem, smem, smem],
        out_specs=vmem,
        scratch_shapes=[
            pltpu.VMEM((levels, rows, lanes), jnp.float32),
            edge, edge, strip, strip, edges, edges, strip, strip,
            pltpu.SemaphoreType.DMA((8,)),
            pltpu.SemaphoreType.DMA((8,)),
        ],
        compiler_params=pltpu.CompilerParams(collective_id=0, has_side_effects=True),
    )(sums, parent_field, relax_rate, zonal_coef, merid_coef)


def on_device(nest_field, nest_area, parent_field, nest_offset, relax_rate, zonal_coef, merid_coef):
    cols = parent_field.shape[2]
    width = chunk_width(cols)
    per_device = cols // width
    partial = front(nest_field, nest_area, nest_offset, width, per_device + 1)
    places = per_device * lax.axis_size("lon")
    sums = lax.switch(
        nest_offset[0] // 3 // width,
        [functools.partial(moved, place=p, per_device=per_device) for p in range(places)],
        partial,
    )
    return tail(sums, parent_field, relax_rate, zonal_coef, merid_coef)


def solution(mesh):
    placed = (P(None, "band", "lon"), P("band", "lon"), P(None, "band", "lon"), P(), P(), P(), P())
    return jax.shard_map(
        on_device, mesh=mesh, in_specs=placed, out_specs=P(None, "band", "lon"), check_vma=False
    )
```

```python
import functools

import jax
import jax.numpy as jnp
from jax import lax
from jax.experimental import pallas as pl
from jax.experimental.pallas import tpu as pltpu
from jax.sharding import PartitionSpec as P

NS = 3
HALO = NS
LANES = 128
GROUP = 4
MESH = pl.DeviceIdType.MESH


def chunk_width(par_cols):
    return max(w for w in range(1, 65) if par_cols % w == 0)


def front_kernel(width, off_ref, nest_ref, area_ref, out_ref, select, sums):
    block = pl.program_id(0)
    per, rows, cols = nest_ref.shape
    chunks = out_ref.shape[0]
    half = out_ref.shape[2]
    offset = off_ref[0]

    def place(values, first, count):
        values = values.reshape(count * rows, cols)
        high = values.astype(jnp.bfloat16)
        low = (values - high.astype(jnp.float32)).astype(jnp.bfloat16)
        by_column = jnp.dot(high, select[...], preferred_element_type=jnp.float32) + jnp.dot(
            low, select[...], preferred_element_type=jnp.float32
        )
        third = count * rows // 3
        tiles = []
        for t in range(sums.shape[0]):
            sums[t, : count * rows] = by_column[:, t * LANES : (t + 1) * LANES]
            tiles.append(
                sums.at[t][pl.ds(0, third, stride=3), :]
                + sums.at[t][pl.ds(1, third, stride=3), :]
                + sums.at[t][pl.ds(2, third, stride=3), :]
            )
        total = jnp.concatenate(tiles, axis=1).reshape(count, 2 * half, LANES * len(tiles))
        for c in range(chunks):
            part = total[:, :, c * width : (c + 1) * width]
            packed = jnp.concatenate([part[:, :half], part[:, half:]], axis=2)
            out_ref[c, pl.ds(first, count)] = packed

    @pl.when(block == 0)
    def _():
        slot = lax.broadcasted_iota(jnp.int32, select.shape, 1)
        cell = lax.broadcasted_iota(jnp.int32, select.shape, 0)
        lowest = (slot - lax.rem(lax.div(offset, 3), width)) * 3 - lax.rem(offset, 3)
        hit = (cell >= lowest) & (cell < lowest + 3)
        select[...] = jnp.where(hit, 1.0, 0.0).astype(jnp.bfloat16)
        place(area_ref[...][None], out_ref.shape[1] - 1, 1)

    place(nest_ref[...] * area_ref[...][None], block * per, per)


def front(nest_field, nest_area, nest_offset, width, chunks):
    levels, rows, cols = nest_field.shape
    half = rows // 6
    per = 8
    tiles = (chunks * width + LANES - 1) // LANES
    return pl.pallas_call(
        functools.partial(front_kernel, width),
        grid=(levels // per,),
        out_shape=jax.ShapeDtypeStruct((chunks, levels + 1, half, 2 * width), jnp.float32),
        in_specs=[
            pl.BlockSpec(memory_space=pltpu.SMEM),
            pl.BlockSpec((per, rows, cols), lambda b: (b, 0, 0)),
            pl.BlockSpec((rows, cols), lambda b: (0, 0)),
        ],
        out_specs=pl.BlockSpec((chunks, levels + 1, half, 2 * width), lambda b: (0, 0, 0, 0)),
        scratch_shapes=[
            pltpu.VMEM((cols, tiles * LANES), jnp.bfloat16),
            pltpu.VMEM((tiles, per * rows, LANES), jnp.float32),
        ],
        compiler_params=pltpu.CompilerParams(dimension_semantics=("arbitrary",)),
    )(nest_offset, nest_field, nest_area)


def send_on(value, steps):
    count = lax.axis_size("lon")
    if steps % count == 0:
        return value
    return lax.ppermute(value, "lon", [(i, (i + steps) % count) for i in range(count)])


def moved(partial, place, per_device):
    steps, slot = divmod(place, per_device)
    near = send_on(partial[: per_device - slot], steps)
    far = send_on(partial[per_device - slot :], steps + 1)
    shared = near[:1] + far[slot:]
    return jnp.concatenate([far[:slot], shared, near[1:]], axis=0)


def blend_kernel(
    sums_ref, parent_ref, relax_ref, field, west_in, east_in, above_in, below_in,
    west_out, east_out, first_out, last_out, west_got, east_got, above_got, below_got,
    send_sems, recv_sems,
):
    lon, band = lax.axis_index("lon"), lax.axis_index("band")
    lons, bands = lax.axis_size("lon"), lax.axis_size("band")
    levels, rows, cols = parent_ref.shape
    lanes = field.shape[2]
    chunks, _, half, double = sums_ref.shape
    width = double // 2
    west, east = lax.rem(lon + lons - 1, lons), lax.rem(lon + 1, lons)
    has_above, has_below = band > 0, band < bands - 1

    barrier = pltpu.get_barrier_semaphore()

    def greet(x, y):
        pl.semaphore_signal(barrier, inc=1, device_id=(x, y), device_id_type=MESH)

    greet(west, band)
    greet(east, band)

    @pl.when(has_above)
    def _():
        for x in (west, lon, east):
            greet(x, band - 1)

    @pl.when(has_below)
    def _():
        for x in (west, lon, east):
            greet(x, band + 1)

    lane = lax.broadcasted_iota(jnp.int32, (rows, LANES), 1)
    at = (cols - HALO) // LANES * LANES
    shares = [1.0 / sums_ref[c, levels] for c in range(chunks)]

    def blend(step, edges):
        west_edge, east_edge = edges
        group = [step * GROUP + g for g in range(GROUP)]
        values = []
        for level in group:
            top, bottom = [], []
            for c in range(chunks):
                ratio = sums_ref[c, level] * shares[c]
                top.append(ratio[:, :width])
                bottom.append(ratio[:, width:])
            restricted = jnp.concatenate(
                [jnp.concatenate(top, axis=1), jnp.concatenate(bottom, axis=1)], axis=0
            )
            parent = parent_ref[level]
            value = parent + relax_ref[level] * (restricted - parent)
            values.append(
                jnp.concatenate([value, jnp.zeros((rows, lanes - cols), jnp.float32)], axis=1)
            )
        for level, value in zip(group, values):
            mine = lane // 4 == level
            west_edge = jnp.where(mine, pltpu.roll(value[:, :LANES], 4 * level, 1), west_edge)
            east_edge = jnp.where(
                mine,
                pltpu.roll(
                    value[:, at : at + LANES],
                    lax.rem(4 * level + LANES - (cols - HALO - at), LANES),
                    1,
                ),
                east_edge,
            )
        for level, value in zip(group, values):
            field[level] = value
            for k in range(HALO):
                first_out[k, pl.ds(level, 1), :] = value[k : k + 1]
                last_out[k, pl.ds(level, 1), :] = value[rows - HALO + k : rows - HALO + k + 1]
        return west_edge, east_edge

    empty = jnp.zeros((rows, LANES), jnp.float32)
    west_edge, east_edge = lax.fori_loop(0, levels // GROUP, blend, (empty, empty))
    west_out[...] = west_edge
    east_out[...] = east_edge

    pl.semaphore_wait(
        barrier, 2 + 3 * has_above.astype(jnp.int32) + 3 * has_below.astype(jnp.int32)
    )

    def copy(index, source, target, x, y):
        return pltpu.make_async_remote_copy(
            src_ref=source,
            dst_ref=target,
            send_sem=send_sems.at[index],
            recv_sem=recv_sems.at[index],
            device_id=(x, y),
            device_id_type=MESH,
        )

    same = [
        copy(0, west_out, east_got.at[0], west, band),
        copy(1, east_out, west_got.at[0], east, band),
    ]
    upward = [
        copy(2, first_out, below_got, lon, band - 1),
        copy(3, west_out, east_got.at[2], west, band - 1),
        copy(4, east_out, west_got.at[2], east, band - 1),
    ]
    downward = [
        copy(5, last_out, above_got, lon, band + 1),
        copy(6, west_out, east_got.at[1], west, band + 1),
        copy(7, east_out, west_got.at[1], east, band + 1),
    ]

    @pl.when(has_above)
    def _():
        for one in upward:
            one.start()

    @pl.when(has_below)
    def _():
        for one in downward:
            one.start()

    for one in same:
        one.start()

    @pl.when(jnp.logical_not(has_above))
    def _():
        above_in[...] = jnp.zeros_like(above_in)
        east_in[1] = empty
        west_in[1] = empty

    @pl.when(jnp.logical_not(has_below))
    def _():
        below_in[...] = jnp.zeros_like(below_in)
        east_in[2] = empty
        west_in[2] = empty

    for one in same:
        one.wait_recv()
    east_in[0] = east_got[0]
    west_in[0] = west_got[0]

    @pl.when(has_above)
    def _():
        for one in downward:
            one.wait_recv()
        above_in[...] = above_got[...]
        east_in[1] = east_got[1]
        west_in[1] = west_got[1]

    @pl.when(has_below)
    def _():
        for one in upward:
            one.wait_recv()
        below_in[...] = below_got[...]
        east_in[2] = east_got[2]
        west_in[2] = west_got[2]

    for one in same:
        one.wait_send()

    @pl.when(has_above)
    def _():
        for one in upward:
            one.wait_send()

    @pl.when(has_below)
    def _():
        for one in downward:
            one.wait_send()


def smooth_kernel(
    field, west_in, east_in, above_in, below_in, zonal_ref, merid_ref, out_ref
):
    band, bands = lax.axis_index("band"), lax.axis_size("band")
    has_above, has_below = band > 0, band < bands - 1
    per, rows, cols = out_ref.shape
    lanes = field.shape[2]
    tall = rows + 8
    sub = lax.broadcasted_iota(jnp.int32, (8, LANES), 0)

    def column_of(ref):
        corner = jnp.where(
            sub < HALO, ref[2, :8], jnp.where(sub >= 8 - HALO, ref[1, rows - 8 :], 0.0)
        )
        return jnp.concatenate([ref[0], corner], axis=0)

    east_cols, west_cols = column_of(east_in), column_of(west_in)
    row = lax.broadcasted_iota(jnp.int32, (tall, lanes), 0)
    valid = (
        (row < rows)
        | ((row < rows + HALO) & has_below)
        | ((row >= tall - HALO) & has_above)
    )
    wide = lax.broadcasted_iota(jnp.int32, (tall, LANES), 1)
    head = lanes - LANES
    spare = jnp.zeros((8 - 2 * HALO, lanes), jnp.float32)
    base = pl.program_id(0) * per

    def smooth(step, carry):
        places = [step * GROUP + g for g in range(GROUP)]
        group = [base + place for place in places]
        values = []
        for level in group:
            extra = [below_in[k, pl.ds(level, 1), :] for k in range(HALO)] + [spare]
            extra += [above_in[k, pl.ds(level, 1), :] for k in range(HALO)]
            value = jnp.concatenate([field[level]] + extra, axis=0)
            right = pltpu.roll(east_cols, lax.rem(cols - head + LANES - 4 * level, LANES), 1)
            left = pltpu.roll(west_cols, lax.rem(2 * LANES - HALO - 4 * level, LANES), 1)
            tile = value[:, head:]
            tile = jnp.where((wide >= cols - head) & (wide < cols - head + HALO), right, tile)
            tile = jnp.where(wide >= LANES - HALO, left, tile)
            if head:
                tile = jnp.concatenate([value[:, :head], tile], axis=1)
            values.append(tile)
        zonal = [zonal_ref[level] for level in group]
        merid = [merid_ref[level] for level in group]
        for sweep in range(NS):
            sides = [pltpu.roll(v, 1, 1) + pltpu.roll(v, lanes - 1, 1) for v in values]
            values = [v + z * (s - 2.0 * v) for v, z, s in zip(values, zonal, sides)]
            sides = [pltpu.roll(v, 1, 0) + pltpu.roll(v, tall - 1, 0) for v in values]
            values = [
                jnp.where(valid, v + m * (s - 2.0 * v), 0.0)
                for v, m, s in zip(values, merid, sides)
            ]
        for place, value in zip(places, values):
            out_ref[place] = value[:rows, :cols]
        return carry

    lax.fori_loop(0, per // GROUP, smooth, 0)


def tail(sums, parent_field, relax_rate, zonal_coef, merid_coef):
    levels, rows, cols = parent_field.shape
    lanes = (cols + 2 * HALO + LANES - 1) // LANES * LANES
    assert 4 * levels <= LANES and cols - (lanes - LANES) >= HALO
    vmem, smem = pl.BlockSpec(memory_space=pltpu.VMEM), pl.BlockSpec(memory_space=pltpu.SMEM)
    kept = [(levels, rows, lanes)] + [(3, rows, LANES)] * 2 + [(HALO, levels, lanes)] * 2
    edge = pltpu.VMEM((rows, LANES), jnp.float32)
    strip = pltpu.VMEM((HALO, levels, lanes), jnp.float32)
    around = pl.pallas_call(
        blend_kernel,
        out_shape=[jax.ShapeDtypeStruct(shape, jnp.float32) for shape in kept],
        in_specs=[vmem, vmem, smem],
        out_specs=[vmem] * 5,
        scratch_shapes=[edge, edge, strip, strip]
        + [pltpu.VMEM(shape, jnp.float32) for shape in kept[1:]]
        + [pltpu.SemaphoreType.DMA((8,)), pltpu.SemaphoreType.DMA((8,))],
        compiler_params=pltpu.CompilerParams(
            collective_id=0, has_side_effects=True, vmem_limit_bytes=16 << 20
        ),
    )(sums, parent_field, relax_rate)
    per = 8
    return pl.pallas_call(
        smooth_kernel,
        grid=(levels // per,),
        out_shape=jax.ShapeDtypeStruct(parent_field.shape, jnp.float32),
        in_specs=[vmem] * 5 + [smem] * 2,
        out_specs=pl.BlockSpec((per, rows, cols), lambda b: (b, 0, 0)),
        compiler_params=pltpu.CompilerParams(
            dimension_semantics=("arbitrary",), vmem_limit_bytes=16 << 20
        ),
    )(*around, zonal_coef, merid_coef)


def on_device(nest_field, nest_area, parent_field, nest_offset, relax_rate, zonal_coef, merid_coef):
    cols = parent_field.shape[2]
    width = chunk_width(cols)
    per_device = cols // width
    partial = front(nest_field, nest_area, nest_offset, width, per_device + 1)
    places = per_device * lax.axis_size("lon")
    sums = lax.switch(
        lax.div(nest_offset[0], 3 * width),
        [functools.partial(moved, place=p, per_device=per_device) for p in range(places)],
        partial,
    )
    return tail(sums, parent_field, relax_rate, zonal_coef, merid_coef)


def solution(mesh):
    placed = (P(None, "band", "lon"), P("band", "lon"), P(None, "band", "lon"), P(), P(), P(), P())
    return jax.shard_map(
        on_device, mesh=mesh, in_specs=placed, out_specs=P(None, "band", "lon"), check_vma=False
    )
```

```python
import functools

import jax
import jax.numpy as jnp
from jax import lax
from jax.experimental import pallas as pl
from jax.experimental.pallas import tpu as pltpu
from jax.sharding import PartitionSpec as P

NS = 3
HALO = NS
LANES = 128
BLEND_GROUP = 16
PASS_GROUP = 8
MESH = pl.DeviceIdType.MESH


def chunk_width(par_cols):
    return max(w for w in range(1, 65) if par_cols % w == 0)


def front_kernel(width, off_ref, nest_ref, area_ref, out_ref, select, sums):
    block = pl.program_id(0)
    per, rows, cols = nest_ref.shape
    chunks = out_ref.shape[0]
    half = out_ref.shape[2]
    offset = off_ref[0]

    def place(values, first, count):
        values = values.reshape(count * rows, cols)
        high = values.astype(jnp.bfloat16)
        low = (values - high.astype(jnp.float32)).astype(jnp.bfloat16)
        by_column = jnp.dot(high, select[...], preferred_element_type=jnp.float32) + jnp.dot(
            low, select[...], preferred_element_type=jnp.float32
        )
        third = count * rows // 3
        tiles = []
        for t in range(sums.shape[0]):
            sums[t, : count * rows] = by_column[:, t * LANES : (t + 1) * LANES]
            tiles.append(
                sums.at[t][pl.ds(0, third, stride=3), :]
                + sums.at[t][pl.ds(1, third, stride=3), :]
                + sums.at[t][pl.ds(2, third, stride=3), :]
            )
        total = jnp.concatenate(tiles, axis=1).reshape(count, 2 * half, LANES * len(tiles))
        for c in range(chunks):
            part = total[:, :, c * width : (c + 1) * width]
            packed = jnp.concatenate([part[:, :half], part[:, half:]], axis=2)
            out_ref[c, pl.ds(first, count)] = packed

    @pl.when(block == 0)
    def _():
        slot = lax.broadcasted_iota(jnp.int32, select.shape, 1)
        cell = lax.broadcasted_iota(jnp.int32, select.shape, 0)
        lowest = (slot - lax.rem(lax.div(offset, 3), width)) * 3 - lax.rem(offset, 3)
        hit = (cell >= lowest) & (cell < lowest + 3)
        select[...] = jnp.where(hit, 1.0, 0.0).astype(jnp.bfloat16)
        place(area_ref[...][None], out_ref.shape[1] - 1, 1)

    place(nest_ref[...] * area_ref[...][None], block * per, per)


def front(nest_field, nest_area, nest_offset, width, chunks):
    levels, rows, cols = nest_field.shape
    half = rows // 6
    per = 8
    tiles = (chunks * width + LANES - 1) // LANES
    return pl.pallas_call(
        functools.partial(front_kernel, width),
        grid=(levels // per,),
        out_shape=jax.ShapeDtypeStruct((chunks, levels + 1, half, 2 * width), jnp.float32),
        in_specs=[
            pl.BlockSpec(memory_space=pltpu.SMEM),
            pl.BlockSpec((per, rows, cols), lambda b: (b, 0, 0)),
            pl.BlockSpec((rows, cols), lambda b: (0, 0)),
        ],
        out_specs=pl.BlockSpec((chunks, levels + 1, half, 2 * width), lambda b: (0, 0, 0, 0)),
        scratch_shapes=[
            pltpu.VMEM((cols, tiles * LANES), jnp.bfloat16),
            pltpu.VMEM((tiles, per * rows, LANES), jnp.float32),
        ],
        compiler_params=pltpu.CompilerParams(dimension_semantics=("arbitrary",)),
    )(nest_offset, nest_field, nest_area)


def move_kernel(steps, slot, part_ref, out_ref, near_got, far_got, send_sems, recv_sems):
    lon, band, lons = lax.axis_index("lon"), lax.axis_index("band"), lax.axis_size("lon")
    own = part_ref.shape[0] - 1 - slot
    jobs = []
    for index, (first, count, got, ahead) in enumerate(
        [(0, own, near_got, steps % lons), (own, slot + 1, far_got, (steps + 1) % lons)]
    ):
        if ahead:
            jobs.append((index, part_ref.at[pl.ds(first, count)], got, ahead))
    barrier = pltpu.get_barrier_semaphore()
    for _, _, _, ahead in jobs:
        for other in (lax.rem(lon + ahead, lons), lax.rem(lon + lons - ahead, lons)):
            pl.semaphore_signal(barrier, inc=1, device_id=(other, band), device_id_type=MESH)
    pl.semaphore_wait(barrier, 2 * len(jobs))
    copies = [
        pltpu.make_async_remote_copy(
            src_ref=source,
            dst_ref=got,
            send_sem=send_sems.at[index],
            recv_sem=recv_sems.at[index],
            device_id=(lax.rem(lon + ahead, lons), band),
            device_id_type=MESH,
        )
        for index, source, got, ahead in jobs
    ]
    for one in copies:
        one.start()
    for one in copies:
        one.wait_recv()
    near = near_got if steps % lons else part_ref.at[pl.ds(0, own)]
    far = far_got if (steps + 1) % lons else part_ref.at[pl.ds(own, slot + 1)]
    for place in range(slot):
        out_ref[place] = far[place]
    out_ref[slot] = near[0] + far[slot]
    for place in range(slot + 1, out_ref.shape[0]):
        out_ref[place] = near[place - slot]
    for one in copies:
        one.wait_send()


def moved(partial, place, per_device):
    steps, slot = divmod(place, per_device)
    plane = partial.shape[1:]
    vmem = pl.BlockSpec(memory_space=pltpu.VMEM)
    return pl.pallas_call(
        functools.partial(move_kernel, steps, slot),
        out_shape=jax.ShapeDtypeStruct((per_device,) + plane, jnp.float32),
        in_specs=[vmem],
        out_specs=vmem,
        scratch_shapes=[
            pltpu.VMEM((per_device - slot,) + plane, jnp.float32),
            pltpu.VMEM((slot + 1,) + plane, jnp.float32),
            pltpu.SemaphoreType.DMA((2,)),
            pltpu.SemaphoreType.DMA((2,)),
        ],
        compiler_params=pltpu.CompilerParams(
            collective_id=1 + place, has_side_effects=True, vmem_limit_bytes=16 << 20
        ),
    )(partial)


def blend_kernel(
    sums_ref, parent_ref, relax_ref, field, west_in, east_in, above_in, below_in,
    west_out, east_out, first_out, last_out, west_got, east_got, above_got, below_got,
    send_sems, recv_sems,
):
    lon, band = lax.axis_index("lon"), lax.axis_index("band")
    lons, bands = lax.axis_size("lon"), lax.axis_size("band")
    levels, rows, cols = parent_ref.shape
    lanes = field.shape[2]
    chunks, _, half, double = sums_ref.shape
    width = double // 2
    west, east = lax.rem(lon + lons - 1, lons), lax.rem(lon + 1, lons)
    has_above, has_below = band > 0, band < bands - 1

    barrier = pltpu.get_barrier_semaphore()

    def greet(x, y):
        pl.semaphore_signal(barrier, inc=1, device_id=(x, y), device_id_type=MESH)

    greet(west, band)
    greet(east, band)

    @pl.when(has_above)
    def _():
        for x in (west, lon, east):
            greet(x, band - 1)

    @pl.when(has_below)
    def _():
        for x in (west, lon, east):
            greet(x, band + 1)

    lane = lax.broadcasted_iota(jnp.int32, (rows, LANES), 1)
    at = (cols - HALO) // LANES * LANES
    shares = [1.0 / sums_ref[c, levels] for c in range(chunks)]

    def blend(step, edges):
        west_edge, east_edge = edges
        group = [step * BLEND_GROUP + g for g in range(BLEND_GROUP)]
        values = []
        for level in group:
            top, bottom = [], []
            for c in range(chunks):
                ratio = sums_ref[c, level] * shares[c]
                top.append(ratio[:, :width])
                bottom.append(ratio[:, width:])
            restricted = jnp.concatenate(
                [jnp.concatenate(top, axis=1), jnp.concatenate(bottom, axis=1)], axis=0
            )
            parent = parent_ref[level]
            value = parent + relax_ref[level] * (restricted - parent)
            values.append(
                jnp.concatenate([value, jnp.zeros((rows, lanes - cols), jnp.float32)], axis=1)
            )
        for level, value in zip(group, values):
            mine = lane // 4 == level
            west_edge = jnp.where(mine, pltpu.roll(value[:, :LANES], 4 * level, 1), west_edge)
            east_edge = jnp.where(
                mine,
                pltpu.roll(
                    value[:, at : at + LANES],
                    lax.rem(4 * level + LANES - (cols - HALO - at), LANES),
                    1,
                ),
                east_edge,
            )
        for level, value in zip(group, values):
            field[level] = value
            for k in range(HALO):
                first_out[k, pl.ds(level, 1), :] = value[k : k + 1]
                last_out[k, pl.ds(level, 1), :] = value[rows - HALO + k : rows - HALO + k + 1]
        return west_edge, east_edge

    empty = jnp.zeros((rows, LANES), jnp.float32)
    west_edge, east_edge = lax.fori_loop(0, levels // BLEND_GROUP, blend, (empty, empty))
    west_out[...] = west_edge
    east_out[...] = east_edge

    pl.semaphore_wait(
        barrier, 2 + 3 * has_above.astype(jnp.int32) + 3 * has_below.astype(jnp.int32)
    )

    def copy(index, source, target, x, y):
        return pltpu.make_async_remote_copy(
            src_ref=source,
            dst_ref=target,
            send_sem=send_sems.at[index],
            recv_sem=recv_sems.at[index],
            device_id=(x, y),
            device_id_type=MESH,
        )

    same = [
        copy(0, west_out, east_got.at[0], west, band),
        copy(1, east_out, west_got.at[0], east, band),
    ]
    upward = [
        copy(2, first_out, below_got, lon, band - 1),
        copy(3, west_out, east_got.at[2], west, band - 1),
        copy(4, east_out, west_got.at[2], east, band - 1),
    ]
    downward = [
        copy(5, last_out, above_got, lon, band + 1),
        copy(6, west_out, east_got.at[1], west, band + 1),
        copy(7, east_out, west_got.at[1], east, band + 1),
    ]

    @pl.when(has_above)
    def _():
        for one in upward:
            one.start()

    @pl.when(has_below)
    def _():
        for one in downward:
            one.start()

    for one in same:
        one.start()

    @pl.when(jnp.logical_not(has_above))
    def _():
        above_in[...] = jnp.zeros_like(above_in)
        east_in[1] = empty
        west_in[1] = empty

    @pl.when(jnp.logical_not(has_below))
    def _():
        below_in[...] = jnp.zeros_like(below_in)
        east_in[2] = empty
        west_in[2] = empty

    for one in same:
        one.wait_recv()
    east_in[0] = east_got[0]
    west_in[0] = west_got[0]

    @pl.when(has_above)
    def _():
        for one in downward:
            one.wait_recv()
        above_in[...] = above_got[...]
        east_in[1] = east_got[1]
        west_in[1] = west_got[1]

    @pl.when(has_below)
    def _():
        for one in upward:
            one.wait_recv()
        below_in[...] = below_got[...]
        east_in[2] = east_got[2]
        west_in[2] = west_got[2]

    for one in same:
        one.wait_send()

    @pl.when(has_above)
    def _():
        for one in upward:
            one.wait_send()

    @pl.when(has_below)
    def _():
        for one in downward:
            one.wait_send()


def smooth_kernel(
    field, west_in, east_in, above_in, below_in, zonal_ref, merid_ref, out_ref
):
    band, bands = lax.axis_index("band"), lax.axis_size("band")
    has_above, has_below = band > 0, band < bands - 1
    per, rows, cols = out_ref.shape
    lanes = field.shape[2]
    tall = rows + 8
    sub = lax.broadcasted_iota(jnp.int32, (8, LANES), 0)

    def column_of(ref):
        corner = jnp.where(
            sub < HALO, ref[2, :8], jnp.where(sub >= 8 - HALO, ref[1, rows - 8 :], 0.0)
        )
        return jnp.concatenate([ref[0], corner], axis=0)

    east_cols, west_cols = column_of(east_in), column_of(west_in)
    row = lax.broadcasted_iota(jnp.int32, (tall, lanes), 0)
    valid = (
        (row < rows)
        | ((row < rows + HALO) & has_below)
        | ((row >= tall - HALO) & has_above)
    )
    wide = lax.broadcasted_iota(jnp.int32, (tall, LANES), 1)
    head = lanes - LANES
    spare = jnp.zeros((8 - 2 * HALO, lanes), jnp.float32)
    base = pl.program_id(0) * per

    def smooth(step, carry):
        places = [step * PASS_GROUP + g for g in range(PASS_GROUP)]
        group = [base + place for place in places]
        values = []
        for level in group:
            extra = [below_in[k, pl.ds(level, 1), :] for k in range(HALO)] + [spare]
            extra += [above_in[k, pl.ds(level, 1), :] for k in range(HALO)]
            value = jnp.concatenate([field[level]] + extra, axis=0)
            right = pltpu.roll(east_cols, lax.rem(cols - head + LANES - 4 * level, LANES), 1)
            left = pltpu.roll(west_cols, lax.rem(2 * LANES - HALO - 4 * level, LANES), 1)
            tile = value[:, head:]
            tile = jnp.where((wide >= cols - head) & (wide < cols - head + HALO), right, tile)
            tile = jnp.where(wide >= LANES - HALO, left, tile)
            if head:
                tile = jnp.concatenate([value[:, :head], tile], axis=1)
            values.append(tile)
        zonal = [zonal_ref[level] for level in group]
        merid = [merid_ref[level] for level in group]
        for sweep in range(NS):
            sides = [pltpu.roll(v, 1, 1) + pltpu.roll(v, lanes - 1, 1) for v in values]
            values = [v + z * (s - 2.0 * v) for v, z, s in zip(values, zonal, sides)]
            sides = [pltpu.roll(v, 1, 0) + pltpu.roll(v, tall - 1, 0) for v in values]
            values = [
                jnp.where(valid, v + m * (s - 2.0 * v), 0.0)
                for v, m, s in zip(values, merid, sides)
            ]
        for place, value in zip(places, values):
            out_ref[place] = value[:rows, :cols]
        return carry

    lax.fori_loop(0, per // PASS_GROUP, smooth, 0)


def tail(sums, parent_field, relax_rate, zonal_coef, merid_coef):
    levels, rows, cols = parent_field.shape
    lanes = (cols + 2 * HALO + LANES - 1) // LANES * LANES
    assert 4 * levels <= LANES and cols - (lanes - LANES) >= HALO
    vmem, smem = pl.BlockSpec(memory_space=pltpu.VMEM), pl.BlockSpec(memory_space=pltpu.SMEM)
    kept = [(levels, rows, lanes)] + [(3, rows, LANES)] * 2 + [(HALO, levels, lanes)] * 2
    edge = pltpu.VMEM((rows, LANES), jnp.float32)
    strip = pltpu.VMEM((HALO, levels, lanes), jnp.float32)
    around = pl.pallas_call(
        blend_kernel,
        out_shape=[jax.ShapeDtypeStruct(shape, jnp.float32) for shape in kept],
        in_specs=[vmem, vmem, smem],
        out_specs=[vmem] * 5,
        scratch_shapes=[edge, edge, strip, strip]
        + [pltpu.VMEM(shape, jnp.float32) for shape in kept[1:]]
        + [pltpu.SemaphoreType.DMA((8,)), pltpu.SemaphoreType.DMA((8,))],
        compiler_params=pltpu.CompilerParams(
            collective_id=0, has_side_effects=True, vmem_limit_bytes=16 << 20
        ),
    )(sums, parent_field, relax_rate)
    per = 8
    return pl.pallas_call(
        smooth_kernel,
        grid=(levels // per,),
        out_shape=jax.ShapeDtypeStruct(parent_field.shape, jnp.float32),
        in_specs=[vmem] * 5 + [smem] * 2,
        out_specs=pl.BlockSpec((per, rows, cols), lambda b: (b, 0, 0)),
        compiler_params=pltpu.CompilerParams(
            dimension_semantics=("arbitrary",), vmem_limit_bytes=16 << 20
        ),
    )(*around, zonal_coef, merid_coef)


def on_device(nest_field, nest_area, parent_field, nest_offset, relax_rate, zonal_coef, merid_coef):
    cols = parent_field.shape[2]
    width = chunk_width(cols)
    per_device = cols // width
    partial = front(nest_field, nest_area, nest_offset, width, per_device + 1)
    places = per_device * lax.axis_size("lon")
    sums = lax.switch(
        lax.div(nest_offset[0], 3 * width),
        [functools.partial(moved, place=p, per_device=per_device) for p in range(places)],
        partial,
    )
    return tail(sums, parent_field, relax_rate, zonal_coef, merid_coef)


def solution(mesh):
    placed = (P(None, "band", "lon"), P("band", "lon"), P(None, "band", "lon"), P(), P(), P(), P())
    return jax.shard_map(
        on_device, mesh=mesh, in_specs=placed, out_specs=P(None, "band", "lon"), check_vma=False
    )
```

```python
import functools

import jax
import jax.numpy as jnp
from jax import lax
from jax.experimental import pallas as pl
from jax.experimental.pallas import tpu as pltpu
from jax.sharding import PartitionSpec as P

NS = 3
HALO = NS
LANES = 128
BLEND_GROUP = 16
PASS_GROUP = 8
MESH = pl.DeviceIdType.MESH


def chunk_width(par_cols):
    return max(w for w in range(1, 65) if par_cols % w == 0)


def front_kernel(width, off_ref, nest_ref, area_ref, out_ref, select, sums):
    block = pl.program_id(0)
    per, rows, cols = nest_ref.shape
    chunks = out_ref.shape[0]
    half = out_ref.shape[2]
    offset = off_ref[0]

    def place(values, first, count):
        values = values.reshape(count * rows, cols)
        high = values.astype(jnp.bfloat16)
        low = (values - high.astype(jnp.float32)).astype(jnp.bfloat16)
        by_column = jnp.dot(high, select[...], preferred_element_type=jnp.float32) + jnp.dot(
            low, select[...], preferred_element_type=jnp.float32
        )
        third = count * rows // 3
        tiles = []
        for t in range(sums.shape[0]):
            sums[t, : count * rows] = by_column[:, t * LANES : (t + 1) * LANES]
            tiles.append(
                sums.at[t][pl.ds(0, third, stride=3), :]
                + sums.at[t][pl.ds(1, third, stride=3), :]
                + sums.at[t][pl.ds(2, third, stride=3), :]
            )
        total = jnp.concatenate(tiles, axis=1).reshape(count, 2 * half, LANES * len(tiles))
        for c in range(chunks):
            part = total[:, :, c * width : (c + 1) * width]
            packed = jnp.concatenate([part[:, :half], part[:, half:]], axis=2)
            out_ref[c, pl.ds(first, count)] = packed

    @pl.when(block == 0)
    def _():
        slot = lax.broadcasted_iota(jnp.int32, select.shape, 1)
        cell = lax.broadcasted_iota(jnp.int32, select.shape, 0)
        lowest = (slot - lax.rem(lax.div(offset, 3), width)) * 3 - lax.rem(offset, 3)
        hit = (cell >= lowest) & (cell < lowest + 3)
        select[...] = jnp.where(hit, 1.0, 0.0).astype(jnp.bfloat16)
        place(area_ref[...][None], out_ref.shape[1] - 1, 1)

    place(nest_ref[...] * area_ref[...][None], block * per, per)


def front(nest_field, nest_area, nest_offset, width, chunks):
    levels, rows, cols = nest_field.shape
    half = rows // 6
    per = 8
    tiles = (chunks * width + LANES - 1) // LANES
    return pl.pallas_call(
        functools.partial(front_kernel, width),
        grid=(levels // per,),
        out_shape=jax.ShapeDtypeStruct((chunks, levels + 1, half, 2 * width), jnp.float32),
        in_specs=[
            pl.BlockSpec(memory_space=pltpu.SMEM),
            pl.BlockSpec((per, rows, cols), lambda b: (b, 0, 0)),
            pl.BlockSpec((rows, cols), lambda b: (0, 0)),
        ],
        out_specs=pl.BlockSpec(memory_space=pltpu.VMEM),
        scratch_shapes=[
            pltpu.VMEM((cols, tiles * LANES), jnp.bfloat16),
            pltpu.VMEM((tiles, per * rows, LANES), jnp.float32),
        ],
        compiler_params=pltpu.CompilerParams(dimension_semantics=("arbitrary",)),
    )(nest_offset, nest_field, nest_area)


def move_kernel(steps, slot, part_ref, out_ref, near_got, far_got, send_sems, recv_sems):
    lon, band, lons = lax.axis_index("lon"), lax.axis_index("band"), lax.axis_size("lon")
    own = part_ref.shape[0] - 1 - slot
    jobs = []
    for index, (first, count, got, ahead) in enumerate(
        [(0, own, near_got, steps % lons), (own, slot + 1, far_got, (steps + 1) % lons)]
    ):
        if ahead:
            jobs.append((index, part_ref.at[pl.ds(first, count)], got, ahead))
    barrier = pltpu.get_barrier_semaphore()
    for _, _, _, ahead in jobs:
        for other in (lax.rem(lon + ahead, lons), lax.rem(lon + lons - ahead, lons)):
            pl.semaphore_signal(barrier, inc=1, device_id=(other, band), device_id_type=MESH)
    pl.semaphore_wait(barrier, 2 * len(jobs))
    copies = [
        pltpu.make_async_remote_copy(
            src_ref=source,
            dst_ref=got,
            send_sem=send_sems.at[index],
            recv_sem=recv_sems.at[index],
            device_id=(lax.rem(lon + ahead, lons), band),
            device_id_type=MESH,
        )
        for index, source, got, ahead in jobs
    ]
    for one in copies:
        one.start()
    for one in copies:
        one.wait_recv()
    near = near_got if steps % lons else part_ref.at[pl.ds(0, own)]
    far = far_got if (steps + 1) % lons else part_ref.at[pl.ds(own, slot + 1)]
    for place in range(slot):
        out_ref[place] = far[place]
    out_ref[slot] = near[0] + far[slot]
    for place in range(slot + 1, out_ref.shape[0]):
        out_ref[place] = near[place - slot]
    for one in copies:
        one.wait_send()


def moved(partial, place, per_device):
    steps, slot = divmod(place, per_device)
    plane = partial.shape[1:]
    vmem = pl.BlockSpec(memory_space=pltpu.VMEM)
    return pl.pallas_call(
        functools.partial(move_kernel, steps, slot),
        out_shape=jax.ShapeDtypeStruct((per_device,) + plane, jnp.float32),
        in_specs=[vmem],
        out_specs=vmem,
        scratch_shapes=[
            pltpu.VMEM((per_device - slot,) + plane, jnp.float32),
            pltpu.VMEM((slot + 1,) + plane, jnp.float32),
            pltpu.SemaphoreType.DMA((2,)),
            pltpu.SemaphoreType.DMA((2,)),
        ],
        compiler_params=pltpu.CompilerParams(
            collective_id=1 + place, has_side_effects=True, vmem_limit_bytes=16 << 20
        ),
    )(partial)


def blend_kernel(
    sums_ref, parent_ref, relax_ref, field, west_in, east_in, above_in, below_in,
    west_out, east_out, first_out, last_out, west_got, east_got, above_got, below_got,
    send_sems, recv_sems,
):
    lon, band = lax.axis_index("lon"), lax.axis_index("band")
    lons, bands = lax.axis_size("lon"), lax.axis_size("band")
    levels, rows, cols = parent_ref.shape
    lanes = field.shape[2]
    chunks, _, half, double = sums_ref.shape
    width = double // 2
    west, east = lax.rem(lon + lons - 1, lons), lax.rem(lon + 1, lons)
    has_above, has_below = band > 0, band < bands - 1

    barrier = pltpu.get_barrier_semaphore()

    def greet(x, y):
        pl.semaphore_signal(barrier, inc=1, device_id=(x, y), device_id_type=MESH)

    greet(west, band)
    greet(east, band)

    @pl.when(has_above)
    def _():
        for x in (west, lon, east):
            greet(x, band - 1)

    @pl.when(has_below)
    def _():
        for x in (west, lon, east):
            greet(x, band + 1)

    lane = lax.broadcasted_iota(jnp.int32, (rows, LANES), 1)
    at = (cols - HALO) // LANES * LANES
    shares = [1.0 / sums_ref[c, levels] for c in range(chunks)]

    def blend(step, edges):
        west_edge, east_edge = edges
        group = [step * BLEND_GROUP + g for g in range(BLEND_GROUP)]
        values = []
        for level in group:
            top, bottom = [], []
            for c in range(chunks):
                ratio = sums_ref[c, level] * shares[c]
                top.append(ratio[:, :width])
                bottom.append(ratio[:, width:])
            restricted = jnp.concatenate(
                [jnp.concatenate(top, axis=1), jnp.concatenate(bottom, axis=1)], axis=0
            )
            parent = parent_ref[level]
            value = parent + relax_ref[level] * (restricted - parent)
            values.append(
                jnp.concatenate([value, jnp.zeros((rows, lanes - cols), jnp.float32)], axis=1)
            )
        for level, value in zip(group, values):
            mine = lane // 4 == level
            west_edge = jnp.where(mine, pltpu.roll(value[:, :LANES], 4 * level, 1), west_edge)
            east_edge = jnp.where(
                mine,
                pltpu.roll(
                    value[:, at : at + LANES],
                    lax.rem(4 * level + LANES - (cols - HALO - at), LANES),
                    1,
                ),
                east_edge,
            )
        for level, value in zip(group, values):
            field[level] = value
            for k in range(HALO):
                first_out[k, pl.ds(level, 1), :] = value[k : k + 1]
                last_out[k, pl.ds(level, 1), :] = value[rows - HALO + k : rows - HALO + k + 1]
        return west_edge, east_edge

    empty = jnp.zeros((rows, LANES), jnp.float32)
    west_edge, east_edge = lax.fori_loop(0, levels // BLEND_GROUP, blend, (empty, empty))
    west_out[...] = west_edge
    east_out[...] = east_edge

    pl.semaphore_wait(
        barrier, 2 + 3 * has_above.astype(jnp.int32) + 3 * has_below.astype(jnp.int32)
    )

    def copy(index, source, target, x, y):
        return pltpu.make_async_remote_copy(
            src_ref=source,
            dst_ref=target,
            send_sem=send_sems.at[index],
            recv_sem=recv_sems.at[index],
            device_id=(x, y),
            device_id_type=MESH,
        )

    same = [
        copy(0, west_out, east_got.at[0], west, band),
        copy(1, east_out, west_got.at[0], east, band),
    ]
    upward = [
        copy(2, first_out, below_got, lon, band - 1),
        copy(3, west_out, east_got.at[2], west, band - 1),
        copy(4, east_out, west_got.at[2], east, band - 1),
    ]
    downward = [
        copy(5, last_out, above_got, lon, band + 1),
        copy(6, west_out, east_got.at[1], west, band + 1),
        copy(7, east_out, west_got.at[1], east, band + 1),
    ]

    @pl.when(has_above)
    def _():
        for one in upward:
            one.start()

    @pl.when(has_below)
    def _():
        for one in downward:
            one.start()

    for one in same:
        one.start()

    @pl.when(jnp.logical_not(has_above))
    def _():
        above_in[...] = jnp.zeros_like(above_in)
        east_in[1] = empty
        west_in[1] = empty

    @pl.when(jnp.logical_not(has_below))
    def _():
        below_in[...] = jnp.zeros_like(below_in)
        east_in[2] = empty
        west_in[2] = empty

    for one in same:
        one.wait_recv()
    east_in[0] = east_got[0]
    west_in[0] = west_got[0]

    @pl.when(has_above)
    def _():
        for one in downward:
            one.wait_recv()
        above_in[...] = above_got[...]
        east_in[1] = east_got[1]
        west_in[1] = west_got[1]

    @pl.when(has_below)
    def _():
        for one in upward:
            one.wait_recv()
        below_in[...] = below_got[...]
        east_in[2] = east_got[2]
        west_in[2] = west_got[2]

    for one in same:
        one.wait_send()

    @pl.when(has_above)
    def _():
        for one in upward:
            one.wait_send()

    @pl.when(has_below)
    def _():
        for one in downward:
            one.wait_send()


def smooth_kernel(
    field, west_in, east_in, above_in, below_in, zonal_ref, merid_ref, out_ref
):
    band, bands = lax.axis_index("band"), lax.axis_size("band")
    has_above, has_below = band > 0, band < bands - 1
    per, rows, cols = out_ref.shape
    lanes = field.shape[2]
    tall = rows + 8
    sub = lax.broadcasted_iota(jnp.int32, (8, LANES), 0)

    def column_of(ref):
        corner = jnp.where(
            sub < HALO, ref[2, :8], jnp.where(sub >= 8 - HALO, ref[1, rows - 8 :], 0.0)
        )
        return jnp.concatenate([ref[0], corner], axis=0)

    east_cols, west_cols = column_of(east_in), column_of(west_in)
    row = lax.broadcasted_iota(jnp.int32, (tall, lanes), 0)
    valid = (
        (row < rows)
        | ((row < rows + HALO) & has_below)
        | ((row >= tall - HALO) & has_above)
    )
    wide = lax.broadcasted_iota(jnp.int32, (tall, LANES), 1)
    head = lanes - LANES
    spare = jnp.zeros((8 - 2 * HALO, lanes), jnp.float32)
    base = pl.program_id(0) * per

    def smooth(step, carry):
        places = [step * PASS_GROUP + g for g in range(PASS_GROUP)]
        group = [base + place for place in places]
        values = []
        for level in group:
            extra = [below_in[k, pl.ds(level, 1), :] for k in range(HALO)] + [spare]
            extra += [above_in[k, pl.ds(level, 1), :] for k in range(HALO)]
            value = jnp.concatenate([field[level]] + extra, axis=0)
            right = pltpu.roll(east_cols, lax.rem(cols - head + LANES - 4 * level, LANES), 1)
            left = pltpu.roll(west_cols, lax.rem(2 * LANES - HALO - 4 * level, LANES), 1)
            tile = value[:, head:]
            tile = jnp.where((wide >= cols - head) & (wide < cols - head + HALO), right, tile)
            tile = jnp.where(wide >= LANES - HALO, left, tile)
            if head:
                tile = jnp.concatenate([value[:, :head], tile], axis=1)
            values.append(tile)
        zonal = [zonal_ref[level] for level in group]
        merid = [merid_ref[level] for level in group]
        for sweep in range(NS):
            sides = [pltpu.roll(v, 1, 1) + pltpu.roll(v, lanes - 1, 1) for v in values]
            values = [v + z * (s - 2.0 * v) for v, z, s in zip(values, zonal, sides)]
            sides = [pltpu.roll(v, 1, 0) + pltpu.roll(v, tall - 1, 0) for v in values]
            values = [
                jnp.where(valid, v + m * (s - 2.0 * v), 0.0)
                for v, m, s in zip(values, merid, sides)
            ]
        for place, value in zip(places, values):
            out_ref[place] = value[:rows, :cols]
        return carry

    lax.fori_loop(0, per // PASS_GROUP, smooth, 0)


def tail(sums, parent_field, relax_rate, zonal_coef, merid_coef):
    levels, rows, cols = parent_field.shape
    lanes = (cols + 2 * HALO + LANES - 1) // LANES * LANES
    assert 4 * levels <= LANES and cols - (lanes - LANES) >= HALO
    vmem, smem = pl.BlockSpec(memory_space=pltpu.VMEM), pl.BlockSpec(memory_space=pltpu.SMEM)
    kept = [(levels, rows, lanes)] + [(3, rows, LANES)] * 2 + [(HALO, levels, lanes)] * 2
    edge = pltpu.VMEM((rows, LANES), jnp.float32)
    strip = pltpu.VMEM((HALO, levels, lanes), jnp.float32)
    around = pl.pallas_call(
        blend_kernel,
        out_shape=[jax.ShapeDtypeStruct(shape, jnp.float32) for shape in kept],
        in_specs=[vmem, vmem, smem],
        out_specs=[vmem] * 5,
        scratch_shapes=[edge, edge, strip, strip]
        + [pltpu.VMEM(shape, jnp.float32) for shape in kept[1:]]
        + [pltpu.SemaphoreType.DMA((8,)), pltpu.SemaphoreType.DMA((8,))],
        compiler_params=pltpu.CompilerParams(
            collective_id=0, has_side_effects=True, vmem_limit_bytes=16 << 20
        ),
    )(sums, parent_field, relax_rate)
    per = 8
    return pl.pallas_call(
        smooth_kernel,
        grid=(levels // per,),
        out_shape=jax.ShapeDtypeStruct(parent_field.shape, jnp.float32),
        in_specs=[vmem] * 5 + [smem] * 2,
        out_specs=pl.BlockSpec((per, rows, cols), lambda b: (b, 0, 0)),
        compiler_params=pltpu.CompilerParams(
            dimension_semantics=("arbitrary",), vmem_limit_bytes=16 << 20
        ),
    )(*around, zonal_coef, merid_coef)


def on_device(nest_field, nest_area, parent_field, nest_offset, relax_rate, zonal_coef, merid_coef):
    cols = parent_field.shape[2]
    width = chunk_width(cols)
    per_device = cols // width
    partial = front(nest_field, nest_area, nest_offset, width, per_device + 1)
    places = per_device * lax.axis_size("lon")
    sums = lax.switch(
        lax.div(nest_offset[0], 3 * width),
        [functools.partial(moved, place=p, per_device=per_device) for p in range(places)],
        partial,
    )
    return tail(sums, parent_field, relax_rate, zonal_coef, merid_coef)


def solution(mesh):
    placed = (P(None, "band", "lon"), P("band", "lon"), P(None, "band", "lon"), P(), P(), P(), P())
    return jax.shard_map(
        on_device, mesh=mesh, in_specs=placed, out_specs=P(None, "band", "lon"), check_vma=False
    )
```
